32 devices in a mesh: groups: 2 (over y), seq: 4 (over z), exp: 2 (over x), rep: 2 (over core).
Axes of the slice: x: 2, y: 2, z: 4, core: 2. Of those that a mesh axis runs over, the one named last changes fastest.
Arguments:
- queries: bfloat16 [512, 4096], P(('groups', 'seq'), ('exp', 'rep')), parts along dimension 0, may hold values from -4 to 4
- key_rows: bfloat16 [512, 4096], P(('groups', 'seq'), ('exp', 'rep')), parts along dimension 0, may hold values from -4 to 4
- value_rows: bfloat16 [512, 4096], P(('groups', 'seq'), ('exp', 'rep')), parts along dimension 0, may hold values from -6 to 6
- decay_log: float32 [512, 32], P(('groups', 'seq'), ('exp', 'rep')), parts along dimension 0, may hold values from -1.5 to 0
- residual: bfloat16 [512, 4096], P(('groups', 'seq'), ('exp', 'rep')), parts along dimension 0, may hold values from -6 to 6
- out_gate: bfloat16 [512, 4096], P(('groups', 'seq'), ('exp', 'rep')), parts along dimension 0, may hold values from -6 to 6
- attn_gain: float32 [4096], P(('exp', 'rep')), may hold values from 0.1 to 1.9
- moe_gain: float32 [4096], P(('exp', 'rep')), may hold values from 0.1 to 1.9
- routes: int32 [512, 2], P(('groups', 'seq')), parts along dimension 0, may hold values from 0 to 31, as said below
- route_weights: float32 [512, 2], P(('groups', 'seq')), parts along dimension 0, may hold values from 0.3 to 1
- w_gate: bfloat16 [2, 4608, 4096], P('exp', 'seq'), may hold values from -0.09375 to 0.09375
- w_up: bfloat16 [2, 4608, 4096], P('exp', 'seq'), may hold values from -0.09375 to 0.09375
- w_down: bfloat16 [2, 4608, 4096], P('exp', 'seq'), may hold values from -0.09375 to 0.09375
Outputs:
- layer_out: bfloat16 [512, 4096], P(('groups', 'seq'), ('exp', 'rep')), parts along dimension 0
The draws below stay inside these ranges and needn't reach their ends.
There are 2 independent parts, one for each index of `groups`. The reference program is written for one: setup_inputs(seed, part) draws one part's arguments, and reference() takes and returns one part's arrays. A program takes and returns all parts, laid end to end along the dimension named above; an argument that names none is the same for every part. Nothing has to cross between parts.
Inputs may be any that keep to these rules, and one draw needn't show every extreme that they name: `routes`: each row names two different experts. Within each aligned block of 64 rows no expert is named by more than 6 rows, every expert is named in every block, and one expert below 2 is named by exactly 6 rows in every block.
All inputs are finite; a program needn't handle non-finite values.
Results may differ from the reference program's by a relative error of at most 0.01.
Values may be sent and summed in bfloat16 or wider, within the bound.
A program may use at most 64 MiB of HBM per device.

```python
from functools import partial
import jax
import jax.numpy as jnp
from jax import lax

HEAD = 128
HEAD_COUNT = 32
D = 4096
FF = 4608
ROUTED = 32
BLOCK = 64
EXPERTS = 2
CAP = 6
L = 256
N_SEQ = 4
N_EXP = 2


def draw_routes(key, part):
    blocks = N_SEQ
    unit = BLOCK // ROUTED
    half_count = ROUTED // 2
    random_subkeys = jax.random.split(jax.random.fold_in(key, 11), 4)
    hot_expert = jax.random.randint(random_subkeys[0], (), 0, N_EXP)
    shifts = jax.random.randint(random_subkeys[1], (blocks, half_count), -unit, unit + 1)
    shifts = jnp.where(jnp.arange(half_count)[None, :] == hot_expert, unit, shifts)
    counts = jnp.concatenate([2 * unit + shifts, 2 * unit - shifts], axis=1)
    bounds = jnp.cumsum(counts, axis=1)
    places = jnp.arange(2 * BLOCK)
    sorted_ids = jnp.sum((bounds[:, None, :] <= places[None, :, None]).astype(jnp.int32), axis=2)

    def shuffle(block_key):
        return jax.random.permutation(block_key, BLOCK)
    orders = jax.vmap(shuffle)(jax.random.split(random_subkeys[2], blocks))
    first_ids = jnp.take_along_axis(sorted_ids, orders, axis=1)
    second_ids = jnp.take_along_axis(sorted_ids, orders + BLOCK, axis=1)
    flips = jax.random.randint(random_subkeys[3], (blocks, BLOCK), 0, 2)
    left_ids = jnp.where(flips == 1, second_ids, first_ids)
    right_ids = jnp.where(flips == 1, first_ids, second_ids)
    return jnp.stack([left_ids, right_ids], axis=2).reshape(blocks * BLOCK, 2).astype(jnp.int32)


def draw_decay_log(key, part):
    sequence_length = BLOCK * N_SEQ
    random_subkeys = jax.random.split(jax.random.fold_in(key, 23), 7)
    fast_share = 0.5
    fast_heads = jax.random.uniform(random_subkeys[0], (HEAD_COUNT,)) < fast_share
    fast_rate = jnp.exp(jax.random.uniform(random_subkeys[1], (HEAD_COUNT,), minval=jnp.log(1.0 / 50.0), maxval=jnp.log(1.0 / 30.0)))
    slow_rate = -jnp.log(jax.random.uniform(random_subkeys[2], (HEAD_COUNT,), minval=0.8, maxval=0.95)) / sequence_length
    rates = jnp.where(fast_heads, fast_rate, slow_rate)
    block_factor = jnp.repeat(jax.random.uniform(random_subkeys[3], (N_SEQ, HEAD_COUNT), minval=0.6, maxval=1.5), BLOCK, axis=0)
    token_factor = jax.random.uniform(random_subkeys[4], (sequence_length, HEAD_COUNT), minval=0.5, maxval=1.5)
    steady_portion = -rates[None, :] * block_factor * token_factor
    surge_position = jax.random.randint(random_subkeys[5], (2, HEAD_COUNT), 0, sequence_length)
    surge_length = jnp.log(jax.random.uniform(random_subkeys[6], (2, HEAD_COUNT), minval=0.5, maxval=0.8))
    token_positions = jnp.arange(sequence_length)[:, None]
    surge_events = jnp.where(token_positions == surge_position[0][None, :], surge_length[0][None, :], 0.0)
    surge_events = surge_events + jnp.where(token_positions == surge_position[1][None, :], surge_length[1][None, :], 0.0)
    return (steady_portion + surge_events).astype(jnp.float32)


def steps_of(stream_key, shape, cuts, least, largest):
    level = 1.0
    for position, blocks in cuts:
        heights = jax.random.uniform(jax.random.fold_in(jax.random.fold_in(stream_key, 6), position), (blocks,), jnp.float32, least / len(cuts), largest / len(cuts))
        level = level * jnp.repeat(jnp.exp(heights), shape[position] // blocks).reshape((-1,) + (1,) * (len(shape) - 1 - position))
    return level


def scatter_about(stream_key, shape, scale, limit, cuts=(), kind=jnp.bfloat16):
    drawn = scale * jax.random.normal(stream_key, shape, jnp.float32)
    if cuts:
        drawn = drawn * steps_of(stream_key, shape, cuts, -0.22, 0.18)
    return jnp.clip(drawn, -limit, limit).astype(kind)


def setup_inputs(seed: int = 0, part: int = 0) -> dict:
    key_of = jax.random.split(jax.random.key(seed), 14)
    own_keys = jax.random.split(jax.random.fold_in(key_of[13], part), 14)
    return {
        "queries": scatter_about(own_keys[0], (L, D), 0.3, 4.0, ((0, 4), (1, 4))),
        "key_rows": scatter_about(own_keys[1], (L, D), 0.3, 4.0, ((0, 4), (1, 4))),
        "value_rows": scatter_about(own_keys[2], (L, D), 1.0, 6.0, ((0, 4), (1, 4))),
        "decay_log": draw_decay_log(jax.random.fold_in(jax.random.fold_in(key_of[13], part), 71), part),
        "residual": scatter_about(own_keys[4], (L, D), 1.0, 6.0, ((0, 4), (1, 4))),
        "out_gate": scatter_about(own_keys[5], (L, D), 1.0, 6.0, ((0, 4), (1, 4))),
        "attn_gain": jnp.clip(1.0 + 0.18 * jax.random.normal(key_of[6], (D,), jnp.float32), 0.1, 1.9),
        "moe_gain": jnp.clip(1.0 + 0.18 * jax.random.normal(key_of[7], (D,), jnp.float32), 0.1, 1.9),
        "routes": draw_routes(jax.random.fold_in(jax.random.fold_in(key_of[13], part), 71), part),
        "route_weights": jnp.clip(0.3 + 0.7 * jax.random.uniform(own_keys[9], (L, 2), jnp.float32) ** steps_of(own_keys[9], (L, 2), ((0, 4),), -0.2, 0.2), 0.3, 1.0),
        "w_gate": scatter_about(key_of[10], (EXPERTS, FF, D), D ** -0.5, 0.09375, ((0, 2), (1, 4))),
        "w_up": scatter_about(key_of[11], (EXPERTS, FF, D), D ** -0.5, 0.09375, ((0, 2), (1, 4))),
        "w_down": scatter_about(key_of[12], (EXPERTS, FF, D), FF ** -0.5, 0.09375, ((0, 2), (1, 4))),
    }


EPSILON = 1e-06

def slot_tables(route_block, weight_block, experts, capacity):
    expert_ids = jnp.arange(experts, dtype=jnp.int32)
    onehot = (route_block[:, :, None] == expert_ids[None, None, :]).astype(jnp.int32)
    tokens = route_block.shape[0]
    flat_hits = onehot.reshape(tokens * 2, experts)
    before = jnp.cumsum(flat_hits, axis=0) - flat_hits
    places = jnp.arange(capacity, dtype=jnp.int32)
    hit_table = flat_hits[:, :, None] * (before[:, :, None] == places[None, None, :]).astype(jnp.int32)
    hit_table = hit_table.astype(jnp.float32).reshape(tokens, 2, experts * capacity)
    dispatch = lax.optimization_barrier(jnp.sum(hit_table, axis=1))
    combine = lax.optimization_barrier(jnp.sum(hit_table * weight_block[:, :, None], axis=1))
    return (dispatch, combine)

def block_attention(carried, inputs):
    query_blk, key_blk, value_blk, decay_blk = inputs
    cumulative = jnp.cumsum(decay_blk, axis=0)
    token_positions = jnp.arange(decay_blk.shape[0])
    causal = (token_positions[:, None] >= token_positions[None, :])[:, :, None]
    log_gaps = cumulative[:, None, :] - cumulative[None, :, :]
    decay_mask = jnp.where(causal, jnp.exp(jnp.where(causal, log_gaps, 0.0)), 0.0)
    scores = jnp.einsum('thd,jhd->htj', query_blk.astype(jnp.float32), key_blk.astype(jnp.float32))
    mixing = (scores * jnp.transpose(decay_mask, (2, 0, 1))).astype(jnp.bfloat16)
    local_part = jnp.einsum('htj,jhd->thd', mixing.astype(jnp.float32), value_blk.astype(jnp.float32))
    lifted = query_blk.astype(jnp.float32) * jnp.exp(cumulative)[:, :, None]
    carried_part = jnp.einsum('thd,hde->the', lifted, carried, precision=lax.Precision.HIGHEST)
    ending = cumulative[-1]
    faded_keys = key_blk.astype(jnp.float32) * jnp.exp(ending[None, :] - cumulative)[:, :, None]
    block_state = jnp.einsum('jhd,jhe->hde', faded_keys, value_blk.astype(jnp.float32), precision=lax.Precision.HIGHEST)
    updated = jnp.exp(ending)[:, None, None] * carried + block_state
    return (updated, local_part + carried_part)

def expert_apply(items):
    slot_rows, gate_mat, up_mat, down_mat = items
    gate_val = jnp.dot(slot_rows, jnp.transpose(gate_mat), preferred_element_type=jnp.float32)
    up_val = jnp.dot(slot_rows, jnp.transpose(up_mat), preferred_element_type=jnp.float32)
    inner_act = (jax.nn.silu(gate_val) * up_val).astype(jnp.bfloat16)
    row_count = slot_rows.shape[0]
    model_width = down_mat.shape[1]
    slab_width = down_mat.shape[0] // N_SEQ
    inner_slabs = jnp.transpose(inner_act.reshape(row_count, N_SEQ, slab_width), (1, 0, 2))
    down_slabs = down_mat.reshape(N_SEQ, slab_width, model_width)

    def add_slab(running, slab_pair):
        slab_out = jnp.dot(slab_pair[0], slab_pair[1], preferred_element_type=jnp.float32).astype(jnp.bfloat16)
        slab_out = lax.optimization_barrier(slab_out)
        return (running + slab_out.astype(jnp.float32), None)
    running, _ = lax.scan(add_slab, jnp.zeros((row_count, model_width), jnp.float32), (inner_slabs, down_slabs))
    return running.astype(jnp.bfloat16)

def reference(queries, key_rows, value_rows, decay_log, residual, out_gate, attn_gain, moe_gain, routes, route_weights, w_gate, w_up, w_down):
    sequence_length = queries.shape[0]
    blocks = sequence_length // BLOCK
    model_width = HEAD_COUNT * HEAD
    query_blocks = queries.reshape(blocks, BLOCK, HEAD_COUNT, HEAD)
    key_blocks = key_rows.reshape(blocks, BLOCK, HEAD_COUNT, HEAD)
    value_blocks = value_rows.reshape(blocks, BLOCK, HEAD_COUNT, HEAD)
    decay_blocks = decay_log.reshape(blocks, BLOCK, HEAD_COUNT)
    start_state = jnp.zeros((HEAD_COUNT, HEAD, HEAD), jnp.float32)
    final_state, mixed_out = lax.scan(block_attention, start_state, (query_blocks, key_blocks, value_blocks, decay_blocks))
    attended = mixed_out.reshape(sequence_length, model_width)
    attn_scale = lax.rsqrt(lax.optimization_barrier(jnp.mean(attended * attended, axis=1, keepdims=True)) + EPSILON)
    hidden = residual.astype(jnp.float32) + jax.nn.sigmoid(out_gate.astype(jnp.float32)) * (attended * attn_scale * attn_gain)
    second = lax.rsqrt(lax.optimization_barrier(jnp.mean(hidden * hidden, axis=1, keepdims=True)) + EPSILON)
    normed = (hidden * second * moe_gain).astype(jnp.bfloat16)
    experts = w_gate.shape[0]
    tables = jax.vmap(partial(slot_tables, experts=experts, capacity=CAP))
    dispatch, combine = tables(routes.reshape(N_SEQ, BLOCK, 2), route_weights.reshape(N_SEQ, BLOCK, 2))
    gathered = jnp.einsum('sbc,sbd->scd', dispatch, normed.reshape(N_SEQ, BLOCK, model_width).astype(jnp.float32)).astype(jnp.bfloat16)
    per_expert = jnp.transpose(gathered.reshape(N_SEQ, experts, CAP, model_width), (1, 0, 2, 3)).reshape(experts, N_SEQ * CAP, model_width)
    outputs = lax.map(expert_apply, (per_expert, w_gate, w_up, w_down))
    returned = jnp.transpose(outputs.reshape(experts, N_SEQ, CAP, model_width), (1, 0, 2, 3)).reshape(N_SEQ, experts * CAP, model_width)
    expert_mix = jnp.einsum('sbc,scd->sbd', combine, returned.astype(jnp.float32), precision=lax.Precision.HIGHEST)
    return (hidden + expert_mix.reshape(sequence_length, model_width)).astype(jnp.bfloat16)
```

```python
import jax
import jax.numpy as jnp
from jax import lax
from jax.experimental import pallas as pl
from jax.experimental.pallas import tpu as pltpu
from jax.sharding import PartitionSpec as P

CAP = 6
SLOTS = 8
EPSILON = 1e-06
MESH = pl.DeviceIdType.MESH
F32 = jnp.float32
BF16 = jnp.bfloat16


def sweep(count, body):
    if count <= 16:
        for i in range(count):
            body(i)
    else:
        lax.fori_loop(0, count, lambda i, c: (body(i), c)[1], 0)


def nt_dot(a, b):
    return lax.dot_general(a, b, (((1,), (1,)), ((), ())), preferred_element_type=F32)


def kernel(
    n_seq,
    n_exp,
    n_rep,
    q_ref,
    k_ref,
    v_ref,
    decay_ref,
    res_ref,
    gate_ref,
    again_ref,
    mgain_ref,
    routes_ref,
    rw_ref,
    wg_hbm,
    wu_hbm,
    wd_hbm,
    out_ref,
    wg,
    wu,
    wd,
    state_in,
    state_out,
    block_state,
    att,
    u_buf,
    sums,
    pack,
    rows,
    xbig,
    half_send,
    half_recv,
    fin,
    back,
    w_sem,
    chain_send,
    chain_recv,
    sums_send,
    sums_recv,
    disp_send,
    disp_recv,
    swap_send,
    swap_recv,
    half_ssem,
    half_rsem,
    back_send,
    back_recv,
):
    z = lax.axis_index("seq")
    x = lax.axis_index("exp")
    r = lax.axis_index("rep")
    other = 1 - r
    tokens, columns = q_ref.shape
    heads = decay_ref.shape[1]
    hd = columns // heads
    hidden_rows = wg.shape[0]
    width = columns * n_exp * n_rep
    whole_rows = wg_hbm.shape[1]

    first = pl.multiple_of(r * hidden_rows, 16) if hidden_rows != whole_rows else 0
    loads = [
        pltpu.make_async_copy(src.at[0, pl.ds(first, hidden_rows), :], dst, w_sem.at[i])
        for i, (src, dst) in enumerate(((wg_hbm, wg), (wu_hbm, wu), (wd_hbm, wd)))
    ]
    for load in loads:
        load.start()

    barrier = pltpu.get_barrier_semaphore()
    plane = n_exp * n_seq

    def greet(i):
        j = i + 1
        pl.semaphore_signal(
            barrier,
            inc=1,
            device_id={
                "exp": lax.rem(x + lax.rem(j, n_exp), n_exp),
                "seq": lax.rem(z + lax.div(j, n_exp), n_seq),
                "rep": r,
            },
            device_id_type=MESH,
        )

    sweep(plane - 1, greet)
    for e in range(n_exp):
        pl.semaphore_signal(
            barrier,
            inc=1,
            device_id={"exp": e, "seq": z, "rep": other},
            device_id_type=MESH,
        )

    ti = lax.broadcasted_iota(jnp.int32, (tokens, tokens), 0)
    tj = lax.broadcasted_iota(jnp.int32, (tokens, tokens), 1)
    causal = ti >= tj
    tri = jnp.where(causal, 1.0, 0.0).astype(F32)
    decay = decay_ref[...]
    cum = jnp.dot(tri, decay, precision=lax.Precision.HIGHEST, preferred_element_type=F32)
    cum_t = jnp.transpose(cum)
    ending = cum[tokens - 1 : tokens, :]
    fading = jnp.exp(ending)
    to_end = jnp.exp(ending - cum)
    lift = jnp.exp(cum)
    for h in range(heads):
        cols = slice(h * hd, (h + 1) * hd)
        faded = k_ref[:, cols].astype(F32) * to_end[:, h : h + 1]
        block_state[h] = jnp.dot(
            jnp.transpose(faded).astype(BF16), v_ref[:, cols], preferred_element_type=F32
        )

    @pl.when(z == 0)
    def _():
        state_in[...] = jnp.zeros_like(state_in)

    pl.semaphore_wait(barrier, plane - 1 + n_exp)

    def hop(h):
        return pltpu.make_async_remote_copy(
            src_ref=state_out.at[h],
            dst_ref=state_in.at[h],
            send_sem=chain_send.at[h],
            recv_sem=chain_recv.at[h],
            device_id={"seq": z + 1},
            device_id_type=MESH,
        )

    @pl.when(z == 0)
    def _():
        for h in range(heads):
            state_out[h] = block_state[h].astype(BF16)
            hop(h).start()

    for h in range(heads):
        cols = slice(h * hd, (h + 1) * hd)
        scores = nt_dot(q_ref[:, cols], k_ref[:, cols])
        gaps = cum[:, h : h + 1] - cum_t[h : h + 1, :]
        mixing = jnp.where(causal, scores * jnp.exp(jnp.where(causal, gaps, 0.0)), 0.0)
        att[:, cols] = jnp.dot(mixing.astype(BF16), v_ref[:, cols], preferred_element_type=F32)

    lane = lax.broadcasted_iota(jnp.int32, (tokens, 128), 1)
    expert_of = lax.div(lane, SLOTS)
    slot_of = lax.rem(lane, SLOTS)
    first_hit = routes_ref[:, 0:1] == expert_of
    second_hit = routes_ref[:, 1:2] == expert_of
    hit = jnp.where(first_hit | second_hit, 1.0, 0.0)
    strict = jnp.where(ti > tj, 1.0, 0.0).astype(BF16)
    before = jnp.dot(strict, hit.astype(BF16), preferred_element_type=F32)
    taken = (hit > 0.5) & (before.astype(jnp.int32) == slot_of) & (slot_of < CAP)
    onehot = jnp.where(taken, 1.0, 0.0)
    combine = jnp.where(first_hit, rw_ref[:, 0:1], rw_ref[:, 1:2]) * onehot
    dispatch = jnp.transpose(onehot)[0 : n_exp * SLOTS, :].astype(BF16)

    for h in range(heads):
        cols = slice(h * hd, (h + 1) * hd)

        @pl.when(z > 0)
        def _():
            hop(h).wait_recv()

            @pl.when(z < n_seq - 1)
            def _():
                state_out[h] = (
                    fading[:, h : h + 1] * state_in[h].astype(F32) + block_state[h]
                ).astype(BF16)
                hop(h).start()

            lifted = (q_ref[:, cols].astype(F32) * lift[:, h : h + 1]).astype(BF16)
            att[:, cols] += jnp.dot(lifted, state_in[h], preferred_element_type=F32)

    res = res_ref[...].astype(F32)
    attended = att[...]
    u = jax.nn.sigmoid(gate_ref[...].astype(F32)) * attended * again_ref[...]
    u_buf[...] = u
    parts = (attended * attended, res * u, u * u, res * res)
    table = jnp.zeros((tokens, 128), F32)
    for i, part in enumerate(parts):
        table = jnp.where(lane == i, jnp.sum(part, axis=1, keepdims=True), table)
    peers = n_exp * n_rep
    me = x * n_rep + r
    sums[me] = jnp.transpose(table)[0:8, :]

    def tell(i):
        to = lax.rem(me + 1 + i, peers)
        pltpu.make_async_remote_copy(
            src_ref=sums.at[me],
            dst_ref=sums.at[me],
            send_sem=sums_send,
            recv_sem=sums_recv,
            device_id={"exp": lax.div(to, n_rep), "rep": lax.rem(to, n_rep)},
            device_id_type=MESH,
        ).start()

    sweep(peers - 1, tell)
    many = sums.at[pl.ds(0, peers - 1)]
    pltpu.make_async_copy(many, many, sums_recv).wait()
    total = jnp.sum(sums[...], axis=0)
    s1 = lax.rsqrt(total[0:1, :] / width + EPSILON)
    moe = total[3:4, :] + s1 * (2.0 * total[1:2, :] + s1 * total[2:3, :])
    s2 = lax.rsqrt(jnp.maximum(moe, 0.0) / width + EPSILON)
    row8 = lax.broadcasted_iota(jnp.int32, (8, tokens), 0)
    scales = jnp.transpose(jnp.where(row8 == 0, s1, s2))
    hidden = res_ref[...].astype(F32) + scales[:, 0:1] * u_buf[...]
    u_buf[...] = hidden
    normed = (hidden * scales[:, 1:2] * mgain_ref[...]).astype(BF16)

    packed = jnp.dot(dispatch, normed, preferred_element_type=F32)
    for e in range(n_exp):
        pack[e] = packed[e * SLOTS : (e + 1) * SLOTS, :].astype(BF16)
    here = x * n_seq + z
    rows[r, here] = pack[x]

    def place(i):
        j = plane - 1 - i
        e = lax.rem(x + lax.rem(j, n_exp), n_exp)
        to = lax.rem(z + lax.div(j, n_exp), n_seq)
        return e, to

    def deal(i):
        e, to = place(i)
        pltpu.make_async_remote_copy(
            src_ref=pack.at[e],
            dst_ref=rows.at[r, here],
            send_sem=disp_send,
            recv_sem=disp_recv,
            device_id={"exp": e, "seq": to},
            device_id_type=MESH,
        ).start()

    sweep(plane - 1, deal)
    arrived = rows.at[r, pl.ds(0, plane - 1)]
    pltpu.make_async_copy(arrived, arrived, disp_recv).wait()
    swap = pltpu.make_async_remote_copy(
        src_ref=rows.at[r],
        dst_ref=rows.at[r],
        send_sem=swap_send,
        recv_sem=swap_recv,
        device_id={"rep": other},
        device_id_type=MESH,
    )
    swap.start()
    for load in loads:
        load.wait()
    slots = n_seq * SLOTS
    swap.wait()
    for s in range(n_rep):
        for e in range(n_exp):
            chunk = rows[s, pl.ds(e * n_seq, n_seq)].astype(F32).reshape(slots, columns)
            at = (e * n_rep + s) * columns
            xbig[:, at : at + columns] = chunk.astype(BF16)

    gate_val = nt_dot(wg[...], xbig[...])
    up_val = nt_dot(wu[...], xbig[...])
    inner = gate_val / (1.0 + jnp.exp(-gate_val)) * up_val
    if hidden_rows == whole_rows:
        unit = lax.broadcasted_iota(jnp.int32, inner.shape, 0)
        inner = jnp.where(lax.div(unit, whole_rows // n_rep) == r, inner, 0.0)
    inner = jnp.transpose(inner).astype(BF16)

    def product(e, s):
        at = pl.multiple_of((e * n_rep + s) * columns, 128)
        return jnp.dot(inner, wd[:, pl.ds(at, columns)], preferred_element_type=F32)

    def half(e):
        return pltpu.make_async_remote_copy(
            src_ref=half_send.at[e],
            dst_ref=half_recv.at[e],
            send_sem=half_ssem.at[e],
            recv_sem=half_rsem.at[e],
            device_id={"rep": other},
            device_id_type=MESH,
        )

    for e in range(n_exp):
        half_send[e] = product(e, other).astype(BF16)
        half(e).start()

    here_back = x * n_seq + z
    for e in range(n_exp):
        own = product(e, r)
        half(e).wait_recv()
        whole = (own + half_recv[e].astype(F32)).reshape(n_seq, SLOTS, columns)
        fin[pl.ds(e * n_seq, n_seq)] = whole.astype(BF16)

    back[here_back] = fin[here_back]

    def hand_back(i):
        e, to = place(i)
        pltpu.make_async_remote_copy(
            src_ref=fin.at[e * n_seq + to],
            dst_ref=back.at[here_back],
            send_sem=back_send,
            recv_sem=back_recv,
            device_id={"exp": e, "seq": to},
            device_id_type=MESH,
        ).start()

    sweep(plane - 1, hand_back)
    returned = back.at[pl.ds(0, plane - 1)]
    pltpu.make_async_copy(returned, returned, back_recv).wait()
    coarse = combine.astype(BF16)
    fine = (combine - coarse.astype(F32)).astype(BF16)
    result = u_buf[...]
    for e in range(n_exp):
        rows_e = jnp.sum(back[pl.ds(e * n_seq, n_seq)].astype(F32), axis=0).astype(BF16)
        lanes = slice(e * SLOTS, (e + 1) * SLOTS)
        result += jnp.dot(coarse[:, lanes], rows_e, preferred_element_type=F32)
        result += jnp.dot(fine[:, lanes], rows_e, preferred_element_type=F32)
    out_ref[...] = result.astype(BF16)

    for h in range(heads):

        @pl.when(z < n_seq - 1)
        def _():
            hop(h).wait_send()

    pltpu.make_async_copy(many, many, sums_send).wait()
    pltpu.make_async_copy(arrived, arrived, disp_send).wait()
    for e in range(n_exp):
        half(e).wait_send()
    pltpu.make_async_copy(returned, returned, back_send).wait()


def solution(mesh):
    n_seq, n_exp, n_rep = (mesh.shape[a] for a in ("seq", "exp", "rep"))

    def shards(
        queries,
        key_rows,
        value_rows,
        decay_log,
        residual,
        out_gate,
        attn_gain,
        moe_gain,
        routes,
        route_weights,
        w_gate,
        w_up,
        w_down,
    ):
        tokens, columns = queries.shape
        heads = decay_log.shape[1]
        hd = columns // heads
        _, whole_rows, width = w_gate.shape
        even = whole_rows % (16 * n_rep) == 0
        hidden_rows = whole_rows // n_rep if even else whole_rows
        plane = n_exp * n_seq
        slots = n_seq * SLOTS
        vmem = pl.BlockSpec(memory_space=pltpu.VMEM)
        hbm = pl.BlockSpec(memory_space=pltpu.HBM)
        dma = pltpu.SemaphoreType.DMA
        return pl.pallas_call(
            lambda *refs: kernel(n_seq, n_exp, n_rep, *refs),
            name="layer",
            out_shape=jax.ShapeDtypeStruct((tokens, columns), BF16),
            in_specs=[vmem] * 10 + [hbm] * 3,
            out_specs=vmem,
            scratch_shapes=[
                pltpu.VMEM((hidden_rows, width), BF16),
                pltpu.VMEM((hidden_rows, width), BF16),
                pltpu.VMEM((hidden_rows, width), BF16),
                pltpu.VMEM((heads, hd, hd), BF16),
                pltpu.VMEM((heads, hd, hd), BF16),
                pltpu.VMEM((heads, hd, hd), F32),
                pltpu.VMEM((tokens, columns), F32),
                pltpu.VMEM((tokens, columns), F32),
                pltpu.VMEM((n_exp * n_rep, 8, tokens), F32),
                pltpu.VMEM((n_exp, SLOTS, columns), BF16),
                pltpu.VMEM((n_rep, plane, SLOTS, columns), BF16),
                pltpu.VMEM((slots, width), BF16),
                pltpu.VMEM((n_exp, slots, columns), BF16),
                pltpu.VMEM((n_exp, slots, columns), BF16),
                pltpu.VMEM((plane, SLOTS, columns), BF16),
                pltpu.VMEM((plane, SLOTS, columns), BF16),
                dma((3,)),
                dma((heads,)),
                dma((heads,)),
                dma,
                dma,
                dma,
                dma,
                dma,
                dma,
                dma((n_exp,)),
                dma((n_exp,)),
                dma,
                dma,
            ],
            compiler_params=pltpu.CompilerParams(collective_id=0, has_side_effects=True),
        )(
            queries,
            key_rows,
            value_rows,
            decay_log,
            residual,
            out_gate,
            attn_gain.reshape(1, columns),
            moe_gain.reshape(1, columns),
            routes,
            route_weights,
            w_gate,
            w_up,
            w_down,
        )

    block = P(("groups", "seq"), ("exp", "rep"))
    gain = P(("exp", "rep"))
    route = P(("groups", "seq"), None)
    weight = P("exp", "seq", None)
    return jax.shard_map(
        shards,
        mesh=mesh,
        in_specs=(block,) * 6 + (gain, gain, route, route) + (weight,) * 3,
        out_specs=block,
        check_vma=False,
    )
```

```python
import jax
import jax.numpy as jnp
from jax import lax
from jax.experimental import pallas as pl
from jax.experimental.pallas import tpu as pltpu
from jax.sharding import PartitionSpec as P

CAP = 6
SLOTS = 8
PARTS = 2
EPSILON = 1e-06
MESH = pl.DeviceIdType.MESH
F32 = jnp.float32
BF16 = jnp.bfloat16


def sweep(count, body):
    if count <= 16:
        for i in range(count):
            body(i)
    else:
        lax.fori_loop(0, count, lambda i, c: (body(i), c)[1], 0)


def nt_dot(a, b):
    return lax.dot_general(a, b, (((1,), (1,)), ((), ())), preferred_element_type=F32)


def kernel(
    n_seq,
    n_exp,
    n_rep,
    k_hbm,
    v_hbm,
    decay_hbm,
    q_hbm,
    routes_hbm,
    rw_hbm,
    res_hbm,
    gate_hbm,
    again_hbm,
    mgain_hbm,
    wg_hbm,
    wu_hbm,
    wd_hbm,
    out_ref,
    k_ref,
    v_ref,
    decay_ref,
    q_ref,
    routes_ref,
    rw_ref,
    res_ref,
    gate_ref,
    again_ref,
    mgain_ref,
    wg,
    wu,
    wd,
    state_in,
    state_out,
    block_state,
    att,
    u_buf,
    sums,
    pack,
    rows,
    half_send,
    half_recv,
    fin,
    back,
    in_sem,
    w_sem,
    up_sem,
    go_sem,
    chain_send,
    chain_recv,
    sums_send,
    sums_recv,
    disp_send,
    disp_recv,
    swap_send,
    swap_recv,
    half_ssem,
    half_rsem,
    back_send,
    back_recv,
):
    z = lax.axis_index("seq")
    x = lax.axis_index("exp")
    r = lax.axis_index("rep")
    other = 1 - r
    tokens, columns = q_ref.shape
    heads = decay_ref.shape[0]
    hd = columns // heads
    part_rows = hd // PARTS
    hidden_rows = wg.shape[0]
    width = columns * n_exp * n_rep
    whole_rows = wg_hbm.shape[1]

    inputs = [
        pltpu.make_async_copy(src, dst, in_sem.at[i])
        for i, (src, dst) in enumerate(
            (
                (k_hbm, k_ref),
                (v_hbm, v_ref),
                (decay_hbm, decay_ref),
                (q_hbm, q_ref),
                (routes_hbm, routes_ref),
                (rw_hbm, rw_ref),
                (res_hbm, res_ref),
                (gate_hbm, gate_ref),
                (again_hbm, again_ref),
                (mgain_hbm, mgain_ref),
            )
        )
    ]
    for load in inputs:
        load.start()
    first = pl.multiple_of(r * hidden_rows, 16) if hidden_rows != whole_rows else 0
    loads = [
        pltpu.make_async_copy(src.at[0, pl.ds(first, hidden_rows), :], dst, w_sem.at[i])
        for i, (src, dst) in enumerate(((wg_hbm, wg), (wu_hbm, wu), (wd_hbm, wd)))
    ]

    barrier = pltpu.get_barrier_semaphore()
    plane = n_exp * n_seq
    peers = n_exp * n_rep
    me = x * n_rep + r
    last = n_seq - 1

    def greet(where):
        pl.semaphore_signal(barrier, inc=1, device_id=where, device_id_type=MESH)

    @pl.when(z < last)
    def _():
        greet({"seq": z + 1})

    @pl.when(z > 0)
    def _():
        greet({"seq": z - 1})

    def greet_peer(i):
        to = lax.rem(me + 1 + i, peers)
        greet({"exp": lax.div(to, n_rep), "rep": lax.rem(to, n_rep)})

    sweep(peers - 1, greet_peer)
    for load in loads:
        load.start()
    for load in inputs[:3]:
        load.wait()

    ti = lax.broadcasted_iota(jnp.int32, (tokens, tokens), 0)
    tj = lax.broadcasted_iota(jnp.int32, (tokens, tokens), 1)
    causal = ti >= tj
    upper = jnp.where(tj >= ti, 1.0, 0.0).astype(F32)
    cum_t = jnp.dot(
        decay_ref[...], upper, precision=lax.Precision.HIGHEST, preferred_element_type=F32
    )
    cum = jnp.transpose(cum_t)
    ending = cum[tokens - 1 : tokens, :]
    fading = jnp.exp(ending)
    to_end = jnp.exp(ending - cum)
    lift = jnp.exp(cum)
    for h in range(heads):
        cols = slice(h * hd, (h + 1) * hd)
        faded = k_ref[:, cols].astype(F32) * to_end[:, h : h + 1]
        block_state[h] = jnp.dot(
            jnp.transpose(faded).astype(BF16), v_ref[:, cols], preferred_element_type=F32
        )

    ends = (z > 0).astype(jnp.int32) + (z < last).astype(jnp.int32)
    pl.semaphore_wait(barrier, peers - 1 + ends)

    def hop(h, p):
        piece = pl.ds(p * part_rows, part_rows)
        return pltpu.make_async_remote_copy(
            src_ref=state_out.at[h, piece],
            dst_ref=state_in.at[h, piece],
            send_sem=chain_send.at[h, p],
            recv_sem=chain_recv.at[h, p],
            device_id={"seq": z + 1},
            device_id_type=MESH,
        )

    @pl.when(z == 0)
    def _():
        for h in range(heads):
            state_out[h] = block_state[h].astype(BF16)
            for p in range(PARTS):
                hop(h, p).start()

    def raise_hand():
        pl.semaphore_signal(up_sem, inc=1, device_id={"seq": z - 1}, device_id_type=MESH)

    @pl.when(z == last)
    def _():
        raise_hand()

    inputs[3].wait()

    for h in range(heads):
        cols = slice(h * hd, (h + 1) * hd)
        scores = nt_dot(q_ref[:, cols], k_ref[:, cols])
        gaps = cum[:, h : h + 1] - cum_t[h : h + 1, :]
        mixing = jnp.where(causal, scores * jnp.exp(jnp.where(causal, gaps, 0.0)), 0.0)
        att[:, cols] = jnp.dot(mixing.astype(BF16), v_ref[:, cols], preferred_element_type=F32)

    @pl.when(z < last)
    def _():
        pl.semaphore_wait(up_sem, 1)

        @pl.when(z > 0)
        def _():
            raise_hand()

    for load in inputs[4:]:
        load.wait()
    lane = lax.broadcasted_iota(jnp.int32, (tokens, 128), 1)
    expert_of = lax.div(lane, SLOTS)
    slot_of = lax.rem(lane, SLOTS)
    named = jnp.transpose(routes_ref[...].astype(F32)).astype(jnp.int32)
    shares = jnp.transpose(rw_ref[...])
    first_hit = named[:, 0:1] == expert_of
    second_hit = named[:, 1:2] == expert_of
    hit = jnp.where(first_hit | second_hit, 1.0, 0.0)
    strict = jnp.where(ti > tj, 1.0, 0.0).astype(BF16)
    before = jnp.dot(strict, hit.astype(BF16), preferred_element_type=F32)
    taken = (hit > 0.5) & (before.astype(jnp.int32) == slot_of) & (slot_of < CAP)
    onehot = jnp.where(taken, 1.0, 0.0)
    combine = jnp.where(first_hit, shares[:, 0:1], shares[:, 1:2]) * onehot
    dispatch = jnp.transpose(onehot)[0 : n_exp * SLOTS, :].astype(BF16)

    def let_go(i):
        pl.semaphore_signal(go_sem, inc=1, device_id={"seq": i}, device_id_type=MESH)

    for h in range(heads):
        cols = slice(h * hd, (h + 1) * hd)

        @pl.when(z > 0)
        def _():
            for p in range(PARTS):
                piece = slice(p * part_rows, (p + 1) * part_rows)
                hop(h, p).wait_recv()

                @pl.when(z < last)
                def _():
                    state_out[h, piece] = (
                        fading[:, h : h + 1] * state_in[h, piece].astype(F32)
                        + block_state[h, piece]
                    ).astype(BF16)
                    hop(h, p).start()

            lifted = (q_ref[:, cols].astype(F32) * lift[:, h : h + 1]).astype(BF16)
            att[:, cols] += jnp.dot(lifted, state_in[h], preferred_element_type=F32)

        if h == max(heads - 3, 0):

            @pl.when(z == last)
            def _():
                sweep(last, let_go)

    res = res_ref[...].astype(F32)
    attended = att[...]
    u = jax.nn.sigmoid(gate_ref[...].astype(F32)) * attended * again_ref[...]
    u_buf[...] = u
    parts = (attended * attended, res * u, u * u, res * res)
    table = jnp.zeros((tokens, 128), F32)
    for i, part in enumerate(parts):
        table = jnp.where(lane == i, jnp.sum(part, axis=1, keepdims=True), table)
    sums[me] = jnp.transpose(table)[0:8, :]

    def tell(i):
        to = lax.rem(me + 1 + i, peers)
        pltpu.make_async_remote_copy(
            src_ref=sums.at[me],
            dst_ref=sums.at[me],
            send_sem=sums_send,
            recv_sem=sums_recv,
            device_id={"exp": lax.div(to, n_rep), "rep": lax.rem(to, n_rep)},
            device_id_type=MESH,
        ).start()

    sweep(peers - 1, tell)
    many = sums.at[pl.ds(0, peers - 1)]
    pltpu.make_async_copy(many, many, sums_recv).wait()
    total = jnp.sum(sums[...], axis=0)
    s1 = lax.rsqrt(total[0:1, :] / width + EPSILON)
    moe = total[3:4, :] + s1 * (2.0 * total[1:2, :] + s1 * total[2:3, :])
    s2 = lax.rsqrt(jnp.maximum(moe, 0.0) / width + EPSILON)
    row8 = lax.broadcasted_iota(jnp.int32, (8, tokens), 0)
    scales = jnp.transpose(jnp.where(row8 == 0, s1, s2))
    hidden = res_ref[...].astype(F32) + scales[:, 0:1] * u_buf[...]
    u_buf[...] = hidden
    normed = (hidden * scales[:, 1:2] * mgain_ref[...]).astype(BF16)

    packed = jnp.dot(dispatch, normed, preferred_element_type=F32)
    for e in range(n_exp):
        pack[e] = packed[e * SLOTS : (e + 1) * SLOTS, :].astype(BF16)
    here = x * n_seq + z
    rows[r, here] = pack[x]

    def deal(e, to, source, target, send_sem, recv_sem):
        pltpu.make_async_remote_copy(
            src_ref=source,
            dst_ref=target,
            send_sem=send_sem,
            recv_sem=recv_sem,
            device_id={"exp": e, "seq": to},
            device_id_type=MESH,
        ).start()

    def deal_rows(e, to):
        deal(e, to, pack.at[e], rows.at[r, here], disp_send, disp_recv)

    def earlier(send):
        def one(i):
            @pl.when(i < z)
            def _():
                for e in range(n_exp):
                    send(e, i)

        sweep(n_seq, one)

    def level(send):
        for j in range(1, n_exp):
            send(lax.rem(x + j, n_exp), z)

    def later(send):
        def one(i):
            @pl.when(last - i > z)
            def _():
                for e in range(n_exp):
                    send(e, last - i)

        sweep(n_seq, one)

    earlier(deal_rows)
    level(deal_rows)

    @pl.when(z < last)
    def _():
        pl.semaphore_wait(go_sem, 1)

    later(deal_rows)
    arrived = rows.at[r, pl.ds(0, plane - 1)]
    pltpu.make_async_copy(arrived, arrived, disp_recv).wait()
    swap = pltpu.make_async_remote_copy(
        src_ref=rows.at[r],
        dst_ref=rows.at[r],
        send_sem=swap_send,
        recv_sem=swap_recv,
        device_id={"rep": other},
        device_id_type=MESH,
    )
    swap.start()
    for load in loads:
        load.wait()
    slots = n_seq * SLOTS

    def project(s):
        gate_part = up_part = 0.0
        for e in range(n_exp):
            chunk = rows[s, pl.ds(e * n_seq, n_seq)].astype(F32).reshape(slots, columns)
            chunk = chunk.astype(BF16)
            at = pl.ds(pl.multiple_of((e * n_rep + s) * columns, 128), columns)
            gate_part += nt_dot(wg[:, at], chunk)
            up_part += nt_dot(wu[:, at], chunk)
        return gate_part, up_part

    gate_val, up_val = project(r)
    swap.wait()
    gate_part, up_part = project(other)
    gate_val += gate_part
    up_val += up_part
    inner = gate_val / (1.0 + jnp.exp(-gate_val)) * up_val
    if hidden_rows == whole_rows:
        unit = lax.broadcasted_iota(jnp.int32, inner.shape, 0)
        inner = jnp.where(lax.div(unit, whole_rows // n_rep) == r, inner, 0.0)
    inner = jnp.transpose(inner).astype(BF16)

    def product(e, s):
        at = pl.multiple_of((e * n_rep + s) * columns, 128)
        return jnp.dot(inner, wd[:, pl.ds(at, columns)], preferred_element_type=F32)

    def half(e):
        return pltpu.make_async_remote_copy(
            src_ref=half_send.at[e],
            dst_ref=half_recv.at[e],
            send_sem=half_ssem.at[e],
            recv_sem=half_rsem.at[e],
            device_id={"rep": other},
            device_id_type=MESH,
        )

    for e in range(n_exp):
        half_send[e] = product(e, other).astype(BF16)
        half(e).start()

    here_back = x * n_seq + z
    for e in range(n_exp):
        own = product(e, r)
        half(e).wait_recv()
        whole = (own + half_recv[e].astype(F32)).reshape(n_seq, SLOTS, columns)
        fin[pl.ds(e * n_seq, n_seq)] = whole.astype(BF16)

    back[here_back] = fin[here_back]

    def hand_back(e, to):
        deal(e, to, fin.at[e * n_seq + to], back.at[here_back], back_send, back_recv)

    earlier(hand_back)
    later(hand_back)
    level(hand_back)
    returned = back.at[pl.ds(0, plane - 1)]
    pltpu.make_async_copy(returned, returned, back_recv).wait()
    coarse = combine.astype(BF16)
    fine = (combine - coarse.astype(F32)).astype(BF16)
    result = u_buf[...]
    for e in range(n_exp):
        rows_e = jnp.sum(back[pl.ds(e * n_seq, n_seq)].astype(F32), axis=0).astype(BF16)
        lanes = slice(e * SLOTS, (e + 1) * SLOTS)
        result += jnp.dot(coarse[:, lanes], rows_e, preferred_element_type=F32)
        result += jnp.dot(fine[:, lanes], rows_e, preferred_element_type=F32)
    out_ref[...] = result.astype(BF16)

    for h in range(heads):

        @pl.when(z < last)
        def _():
            for p in range(PARTS):
                hop(h, p).wait_send()

    pltpu.make_async_copy(many, many, sums_send).wait()
    pltpu.make_async_copy(arrived, arrived, disp_send).wait()
    for e in range(n_exp):
        half(e).wait_send()
    pltpu.make_async_copy(returned, returned, back_send).wait()


def solution(mesh):
    n_seq, n_exp, n_rep = (mesh.shape[a] for a in ("seq", "exp", "rep"))

    def shards(
        queries,
        key_rows,
        value_rows,
        decay_log,
        residual,
        out_gate,
        attn_gain,
        moe_gain,
        routes,
        route_weights,
        w_gate,
        w_up,
        w_down,
    ):
        tokens, columns = queries.shape
        heads = decay_log.shape[1]
        hd = columns // heads
        _, whole_rows, width = w_gate.shape
        even = whole_rows % (16 * n_rep) == 0
        hidden_rows = whole_rows // n_rep if even else whole_rows
        plane = n_exp * n_seq
        slots = n_seq * SLOTS
        vmem = pl.BlockSpec(memory_space=pltpu.VMEM)
        hbm = pl.BlockSpec(memory_space=pltpu.HBM)
        dma = pltpu.SemaphoreType.DMA
        return pl.pallas_call(
            lambda *refs: kernel(n_seq, n_exp, n_rep, *refs),
            name="layer",
            out_shape=jax.ShapeDtypeStruct((tokens, columns), BF16),
            in_specs=[hbm] * 13,
            out_specs=vmem,
            scratch_shapes=[
                pltpu.VMEM((tokens, columns), BF16),
                pltpu.VMEM((tokens, columns), BF16),
                pltpu.VMEM((heads, tokens), F32),
                pltpu.VMEM((tokens, columns), BF16),
                pltpu.VMEM((2, tokens), jnp.int32),
                pltpu.VMEM((2, tokens), F32),
                pltpu.VMEM((tokens, columns), BF16),
                pltpu.VMEM((tokens, columns), BF16),
                pltpu.VMEM((1, columns), F32),
                pltpu.VMEM((1, columns), F32),
                pltpu.VMEM((hidden_rows, width), BF16),
                pltpu.VMEM((hidden_rows, width), BF16),
                pltpu.VMEM((hidden_rows, width), BF16),
                pltpu.VMEM((heads, hd, hd), BF16),
                pltpu.VMEM((heads, hd, hd), BF16),
                pltpu.VMEM((heads, hd, hd), F32),
                pltpu.VMEM((tokens, columns), F32),
                pltpu.VMEM((tokens, columns), F32),
                pltpu.VMEM((n_exp * n_rep, 8, tokens), F32),
                pltpu.VMEM((n_exp, SLOTS, columns), BF16),
                pltpu.VMEM((n_rep, plane, SLOTS, columns), BF16),
                pltpu.VMEM((n_exp, slots, columns), BF16),
                pltpu.VMEM((n_exp, slots, columns), BF16),
                pltpu.VMEM((plane, SLOTS, columns), BF16),
                pltpu.VMEM((plane, SLOTS, columns), BF16),
                dma((10,)),
                dma((3,)),
                pltpu.SemaphoreType.REGULAR,
                pltpu.SemaphoreType.REGULAR,
                dma((heads, PARTS)),
                dma((heads, PARTS)),
                dma,
                dma,
                dma,
                dma,
                dma,
                dma,
                dma((n_exp,)),
                dma((n_exp,)),
                dma,
                dma,
            ],
            compiler_params=pltpu.CompilerParams(collective_id=0, has_side_effects=True),
        )(
            key_rows,
            value_rows,
            decay_log.T,
            queries,
            routes.T,
            route_weights.T,
            residual,
            out_gate,
            attn_gain.reshape(1, columns),
            moe_gain.reshape(1, columns),
            w_gate,
            w_up,
            w_down,
        )

    block = P(("groups", "seq"), ("exp", "rep"))
    gain = P(("exp", "rep"))
    route = P(("groups", "seq"), None)
    weight = P("exp", "seq", None)
    return jax.shard_map(
        shards,
        mesh=mesh,
        in_specs=(block,) * 6 + (gain, gain, route, route) + (weight,) * 3,
        out_specs=block,
        check_vma=False,
    )
```

```python
import jax
import jax.numpy as jnp
from jax import lax
from jax.experimental import pallas as pl
from jax.experimental.pallas import tpu as pltpu
from jax.sharding import PartitionSpec as P

CAP = 6
SLOTS = 8
PARTS = 2
EPSILON = 1e-06
MESH = pl.DeviceIdType.MESH
F32 = jnp.float32
BF16 = jnp.bfloat16


def sweep(count, body):
    if count <= 16:
        for i in range(count):
            body(i)
    else:
        lax.fori_loop(0, count, lambda i, c: (body(i), c)[1], 0)


def nt_dot(a, b):
    return lax.dot_general(a, b, (((1,), (1,)), ((), ())), preferred_element_type=F32)


def kernel(
    n_seq,
    n_exp,
    n_rep,
    k_hbm,
    v_hbm,
    decay_hbm,
    q_hbm,
    routes_hbm,
    rw_hbm,
    res_hbm,
    gate_hbm,
    again_hbm,
    mgain_hbm,
    wg_hbm,
    wu_hbm,
    wd_hbm,
    out_ref,
    k_ref,
    v_ref,
    decay_ref,
    q_ref,
    routes_ref,
    rw_ref,
    res_ref,
    gate_ref,
    again_ref,
    mgain_ref,
    wg,
    wu,
    wd,
    state_in,
    state_out,
    block_state,
    att,
    u_buf,
    sums,
    pack,
    rows,
    half_send,
    half_recv,
    fin,
    back,
    in_sem,
    w_sem,
    go_sem,
    chain_send,
    chain_recv,
    sums_send,
    sums_recv,
    disp_send,
    disp_recv,
    swap_send,
    swap_recv,
    half_ssem,
    half_rsem,
    back_send,
    back_recv,
):
    z = lax.axis_index("seq")
    x = lax.axis_index("exp")
    r = lax.axis_index("rep")
    other = 1 - r
    tokens, columns = q_ref.shape
    heads = decay_ref.shape[0]
    hd = columns // heads
    part_rows = hd // PARTS
    hidden_rows = wg.shape[0]
    width = columns * n_exp * n_rep
    whole_rows = wg_hbm.shape[1]

    inputs = [
        pltpu.make_async_copy(src, dst, in_sem.at[i])
        for i, (src, dst) in enumerate(
            (
                (k_hbm, k_ref),
                (v_hbm, v_ref),
                (decay_hbm, decay_ref),
                (q_hbm, q_ref),
                (routes_hbm, routes_ref),
                (rw_hbm, rw_ref),
                (res_hbm, res_ref),
                (gate_hbm, gate_ref),
                (again_hbm, again_ref),
                (mgain_hbm, mgain_ref),
            )
        )
    ]
    for load in inputs:
        load.start()
    first = pl.multiple_of(r * hidden_rows, 16) if hidden_rows != whole_rows else 0
    loads = [
        pltpu.make_async_copy(src.at[0, pl.ds(first, hidden_rows), :], dst, w_sem.at[i])
        for i, (src, dst) in enumerate(((wg_hbm, wg), (wu_hbm, wu), (wd_hbm, wd)))
    ]

    barrier = pltpu.get_barrier_semaphore()
    plane = n_exp * n_seq
    peers = n_exp * n_rep
    me = x * n_rep + r
    last = n_seq - 1

    def greet(where):
        pl.semaphore_signal(barrier, inc=1, device_id=where, device_id_type=MESH)

    @pl.when(z < last)
    def _():
        greet({"seq": z + 1})

    @pl.when(z > 0)
    def _():
        greet({"seq": z - 1})

    def greet_peer(i):
        to = lax.rem(me + 1 + i, peers)
        greet({"exp": lax.div(to, n_rep), "rep": lax.rem(to, n_rep)})

    sweep(peers - 1, greet_peer)
    for load in loads:
        load.start()
    for load in inputs[:3]:
        load.wait()

    ti = lax.broadcasted_iota(jnp.int32, (tokens, tokens), 0)
    tj = lax.broadcasted_iota(jnp.int32, (tokens, tokens), 1)
    causal = ti >= tj
    upper = jnp.where(tj >= ti, 1.0, 0.0).astype(F32)
    cum_t = jnp.dot(
        decay_ref[...], upper, precision=lax.Precision.HIGHEST, preferred_element_type=F32
    )
    cum = jnp.transpose(cum_t)
    ending = cum[tokens - 1 : tokens, :]
    fading = jnp.exp(ending)
    to_end = jnp.exp(ending - cum)
    lift = jnp.exp(cum)
    for h in range(heads):
        cols = slice(h * hd, (h + 1) * hd)
        faded = k_ref[:, cols].astype(F32) * to_end[:, h : h + 1]
        block_state[h] = jnp.dot(
            jnp.transpose(faded).astype(BF16), v_ref[:, cols], preferred_element_type=F32
        )

    ends = (z > 0).astype(jnp.int32) + (z < last).astype(jnp.int32)
    pl.semaphore_wait(barrier, peers - 1 + ends)

    def hop(h, p):
        piece = pl.ds(p * part_rows, part_rows)
        return pltpu.make_async_remote_copy(
            src_ref=state_out.at[h, piece],
            dst_ref=state_in.at[h, piece],
            send_sem=chain_send.at[h, p],
            recv_sem=chain_recv.at[h, p],
            device_id={"seq": z + 1},
            device_id_type=MESH,
        )

    @pl.when(z == 0)
    def _():
        for h in range(heads):
            state_out[h] = block_state[h].astype(BF16)
            for p in range(PARTS):
                hop(h, p).start()

    inputs[3].wait()

    for h in range(heads):
        cols = slice(h * hd, (h + 1) * hd)
        scores = nt_dot(q_ref[:, cols], k_ref[:, cols])
        gaps = cum[:, h : h + 1] - cum_t[h : h + 1, :]
        mixing = jnp.where(causal, scores * jnp.exp(jnp.where(causal, gaps, 0.0)), 0.0)
        att[:, cols] = jnp.dot(mixing.astype(BF16), v_ref[:, cols], preferred_element_type=F32)

    for load in inputs[4:]:
        load.wait()
    lane = lax.broadcasted_iota(jnp.int32, (tokens, 128), 1)
    expert_of = lax.div(lane, SLOTS)
    slot_of = lax.rem(lane, SLOTS)
    named = jnp.transpose(routes_ref[...].astype(F32)).astype(jnp.int32)
    shares = jnp.transpose(rw_ref[...])
    first_hit = named[:, 0:1] == expert_of
    second_hit = named[:, 1:2] == expert_of
    hit = jnp.where(first_hit | second_hit, 1.0, 0.0)
    strict = jnp.where(ti > tj, 1.0, 0.0).astype(BF16)
    before = jnp.dot(strict, hit.astype(BF16), preferred_element_type=F32)
    taken = (hit > 0.5) & (before.astype(jnp.int32) == slot_of) & (slot_of < CAP)
    onehot = jnp.where(taken, 1.0, 0.0)
    combine = jnp.where(first_hit, shares[:, 0:1], shares[:, 1:2]) * onehot
    dispatch = jnp.transpose(onehot)[0 : n_exp * SLOTS, :].astype(BF16)

    def let_go(i):
        pl.semaphore_signal(go_sem, inc=1, device_id={"seq": i}, device_id_type=MESH)

    for h in range(heads):
        cols = slice(h * hd, (h + 1) * hd)

        @pl.when(z > 0)
        def _():
            for p in range(PARTS):
                piece = slice(p * part_rows, (p + 1) * part_rows)
                hop(h, p).wait_recv()

                @pl.when(z < last)
                def _():
                    state_out[h, piece] = (
                        fading[:, h : h + 1] * state_in[h, piece].astype(F32)
                        + block_state[h, piece]
                    ).astype(BF16)
                    hop(h, p).start()

            lifted = (q_ref[:, cols].astype(F32) * lift[:, h : h + 1]).astype(BF16)
            att[:, cols] += jnp.dot(lifted, state_in[h], preferred_element_type=F32)

        if h == max(heads - 3, 0):

            @pl.when(z == last)
            def _():
                sweep(last, let_go)

    res = res_ref[...].astype(F32)
    attended = att[...]
    u = jax.nn.sigmoid(gate_ref[...].astype(F32)) * attended * again_ref[...]
    u_buf[...] = u
    parts = (attended * attended, res * u, u * u, res * res)
    table = jnp.zeros((tokens, 128), F32)
    for i, part in enumerate(parts):
        table = jnp.where(lane == i, jnp.sum(part, axis=1, keepdims=True), table)
    sums[me] = jnp.transpose(table)[0:8, :]

    def tell(i):
        to = lax.rem(me + 1 + i, peers)
        pltpu.make_async_remote_copy(
            src_ref=sums.at[me],
            dst_ref=sums.at[me],
            send_sem=sums_send,
            recv_sem=sums_recv,
            device_id={"exp": lax.div(to, n_rep), "rep": lax.rem(to, n_rep)},
            device_id_type=MESH,
        ).start()

    sweep(peers - 1, tell)
    many = sums.at[pl.ds(0, peers - 1)]
    pltpu.make_async_copy(many, many, sums_recv).wait()
    total = jnp.sum(sums[...], axis=0)
    s1 = lax.rsqrt(total[0:1, :] / width + EPSILON)
    moe = total[3:4, :] + s1 * (2.0 * total[1:2, :] + s1 * total[2:3, :])
    s2 = lax.rsqrt(jnp.maximum(moe, 0.0) / width + EPSILON)
    row8 = lax.broadcasted_iota(jnp.int32, (8, tokens), 0)
    scales = jnp.transpose(jnp.where(row8 == 0, s1, s2))
    hidden = res_ref[...].astype(F32) + scales[:, 0:1] * u_buf[...]
    u_buf[...] = hidden
    normed = (hidden * scales[:, 1:2] * mgain_ref[...]).astype(BF16)

    packed = jnp.dot(dispatch, normed, preferred_element_type=F32)
    for e in range(n_exp):
        pack[e] = packed[e * SLOTS : (e + 1) * SLOTS, :].astype(BF16)
    here = x * n_seq + z
    rows[r, here] = pack[x]

    def deal(e, to, source, target, send_sem, recv_sem):
        pltpu.make_async_remote_copy(
            src_ref=source,
            dst_ref=target,
            send_sem=send_sem,
            recv_sem=recv_sem,
            device_id={"exp": e, "seq": to},
            device_id_type=MESH,
        ).start()

    def deal_rows(e, to):
        used = pl.ds(0, CAP)
        deal(e, to, pack.at[e, used], rows.at[r, here, used], disp_send, disp_recv)

    def earlier(send):
        def one(i):
            @pl.when(i < z)
            def _():
                for e in range(n_exp):
                    send(e, i)

        sweep(n_seq, one)

    def level(send):
        for j in range(1, n_exp):
            send(lax.rem(x + j, n_exp), z)

    def later(send):
        def one(i):
            @pl.when(last - i > z)
            def _():
                for e in range(n_exp):
                    send(e, last - i)

        sweep(n_seq, one)

    earlier(deal_rows)
    level(deal_rows)

    @pl.when(z < last)
    def _():
        pl.semaphore_wait(go_sem, 1)

    later(deal_rows)
    arrived = rows.at[r, pl.ds(0, plane - 1), pl.ds(0, CAP)]
    pltpu.make_async_copy(arrived, arrived, disp_recv).wait()
    swap = pltpu.make_async_remote_copy(
        src_ref=rows.at[r],
        dst_ref=rows.at[r],
        send_sem=swap_send,
        recv_sem=swap_recv,
        device_id={"rep": other},
        device_id_type=MESH,
    )
    swap.start()
    for load in loads:
        load.wait()
    slots = n_seq * SLOTS

    def project(s):
        gate_part = up_part = 0.0
        for e in range(n_exp):
            chunk = rows[s, pl.ds(e * n_seq, n_seq)].astype(F32).reshape(slots, columns)
            chunk = chunk.astype(BF16)
            at = pl.ds(pl.multiple_of((e * n_rep + s) * columns, 128), columns)
            gate_part += nt_dot(wg[:, at], chunk)
            up_part += nt_dot(wu[:, at], chunk)
        return gate_part, up_part

    gate_val, up_val = project(r)
    swap.wait()
    gate_part, up_part = project(other)
    gate_val += gate_part
    up_val += up_part
    inner = gate_val / (1.0 + jnp.exp(-gate_val)) * up_val
    if hidden_rows == whole_rows:
        unit = lax.broadcasted_iota(jnp.int32, inner.shape, 0)
        inner = jnp.where(lax.div(unit, whole_rows // n_rep) == r, inner, 0.0)
    inner = jnp.transpose(inner).astype(BF16)

    def product(e, s):
        at = pl.multiple_of((e * n_rep + s) * columns, 128)
        return jnp.dot(inner, wd[:, pl.ds(at, columns)], preferred_element_type=F32)

    def half(e):
        return pltpu.make_async_remote_copy(
            src_ref=half_send.at[e],
            dst_ref=half_recv.at[e],
            send_sem=half_ssem.at[e],
            recv_sem=half_rsem.at[e],
            device_id={"rep": other},
            device_id_type=MESH,
        )

    for e in range(n_exp):
        half_send[e] = product(e, other).astype(BF16)
        half(e).start()

    here_back = x * n_seq + z
    for e in range(n_exp):
        own = product(e, r)
        half(e).wait_recv()
        whole = (own + half_recv[e].astype(F32)).reshape(n_seq, SLOTS, columns)
        fin[pl.ds(e * n_seq, n_seq)] = whole.astype(BF16)

    back[here_back] = fin[here_back]

    def hand_back(e, to):
        used = pl.ds(0, CAP)
        source = fin.at[e * n_seq + to, used]
        deal(e, to, source, back.at[here_back, used], back_send, back_recv)

    earlier(hand_back)
    later(hand_back)
    level(hand_back)
    returned = back.at[pl.ds(0, plane - 1), pl.ds(0, CAP)]
    pltpu.make_async_copy(returned, returned, back_recv).wait()
    coarse = combine.astype(BF16)
    fine = (combine - coarse.astype(F32)).astype(BF16)
    result = u_buf[...]
    for e in range(n_exp):
        rows_e = jnp.sum(back[pl.ds(e * n_seq, n_seq)].astype(F32), axis=0)
        slot = lax.broadcasted_iota(jnp.int32, rows_e.shape, 0)
        rows_e = jnp.where(slot < CAP, rows_e, 0.0).astype(BF16)
        lanes = slice(e * SLOTS, (e + 1) * SLOTS)
        result += jnp.dot(coarse[:, lanes], rows_e, preferred_element_type=F32)
        result += jnp.dot(fine[:, lanes], rows_e, preferred_element_type=F32)
    out_ref[...] = result.astype(BF16)

    for h in range(heads):

        @pl.when(z < last)
        def _():
            for p in range(PARTS):
                hop(h, p).wait_send()

    pltpu.make_async_copy(many, many, sums_send).wait()
    pltpu.make_async_copy(arrived, arrived, disp_send).wait()
    for e in range(n_exp):
        half(e).wait_send()
    pltpu.make_async_copy(returned, returned, back_send).wait()


def solution(mesh):
    n_seq, n_exp, n_rep = (mesh.shape[a] for a in ("seq", "exp", "rep"))

    def shards(
        queries,
        key_rows,
        value_rows,
        decay_log,
        residual,
        out_gate,
        attn_gain,
        moe_gain,
        routes,
        route_weights,
        w_gate,
        w_up,
        w_down,
    ):
        tokens, columns = queries.shape
        heads = decay_log.shape[1]
        hd = columns // heads
        _, whole_rows, width = w_gate.shape
        even = whole_rows % (16 * n_rep) == 0
        hidden_rows = whole_rows // n_rep if even else whole_rows
        plane = n_exp * n_seq
        slots = n_seq * SLOTS
        vmem = pl.BlockSpec(memory_space=pltpu.VMEM)
        hbm = pl.BlockSpec(memory_space=pltpu.HBM)
        dma = pltpu.SemaphoreType.DMA
        return pl.pallas_call(
            lambda *refs: kernel(n_seq, n_exp, n_rep, *refs),
            name="layer",
            out_shape=jax.ShapeDtypeStruct((tokens, columns), BF16),
            in_specs=[hbm] * 13,
            out_specs=vmem,
            scratch_shapes=[
                pltpu.VMEM((tokens, columns), BF16),
                pltpu.VMEM((tokens, columns), BF16),
                pltpu.VMEM((heads, tokens), F32),
                pltpu.VMEM((tokens, columns), BF16),
                pltpu.VMEM((2, tokens), jnp.int32),
                pltpu.VMEM((2, tokens), F32),
                pltpu.VMEM((tokens, columns), BF16),
                pltpu.VMEM((tokens, columns), BF16),
                pltpu.VMEM((1, columns), F32),
                pltpu.VMEM((1, columns), F32),
                pltpu.VMEM((hidden_rows, width), BF16),
                pltpu.VMEM((hidden_rows, width), BF16),
                pltpu.VMEM((hidden_rows, width), BF16),
                pltpu.VMEM((heads, hd, hd), BF16),
                pltpu.VMEM((heads, hd, hd), BF16),
                pltpu.VMEM((heads, hd, hd), F32),
                pltpu.VMEM((tokens, columns), F32),
                pltpu.VMEM((tokens, columns), F32),
                pltpu.VMEM((n_exp * n_rep, 8, tokens), F32),
                pltpu.VMEM((n_exp, SLOTS, columns), BF16),
                pltpu.VMEM((n_rep, plane, SLOTS, columns), BF16),
                pltpu.VMEM((n_exp, slots, columns), BF16),
                pltpu.VMEM((n_exp, slots, columns), BF16),
                pltpu.VMEM((plane, SLOTS, columns), BF16),
                pltpu.VMEM((plane, SLOTS, columns), BF16),
                dma((10,)),
                dma((3,)),
                pltpu.SemaphoreType.REGULAR,
                dma((heads, PARTS)),
                dma((heads, PARTS)),
                dma,
                dma,
                dma,
                dma,
                dma,
                dma,
                dma((n_exp,)),
                dma((n_exp,)),
                dma,
                dma,
            ],
            compiler_params=pltpu.CompilerParams(collective_id=0, has_side_effects=True),
        )(
            key_rows,
            value_rows,
            decay_log.T,
            queries,
            routes.T,
            route_weights.T,
            residual,
            out_gate,
            attn_gain.reshape(1, columns),
            moe_gain.reshape(1, columns),
            w_gate,
            w_up,
            w_down,
        )

    block = P(("groups", "seq"), ("exp", "rep"))
    gain = P(("exp", "rep"))
    route = P(("groups", "seq"), None)
    weight = P("exp", "seq", None)
    return jax.shard_map(
        shards,
        mesh=mesh,
        in_specs=(block,) * 6 + (gain, gain, route, route) + (weight,) * 3,
        out_specs=block,
        check_vma=False,
    )
```
